32 devices in a mesh: dp: 16 (over z, y, x), sub: 2 (over core).
Axes of the slice: x: 2, y: 2, z: 4, core: 2. Of those that a mesh axis runs over, the one named last changes fastest.
Arguments:
- projections: float32 [6144, 128], P(('dp', 'sub')), may hold values from -6 to 6
- partner: int32 [6144], P(('dp', 'sub')), may hold values from 0 to 6143, as said below
Outputs:
- loss: float32 [], replicated
- grad_projections: float32 [6144, 128], P(('dp', 'sub'))
The draws below stay inside these ranges and needn't reach their ends.
Inputs may be any that keep to these rules, and one draw needn't show every extreme that they name: partner pairs the views: partner[partner[i]] = i and partner[i] != i for every view.
All inputs are finite; a program needn't handle non-finite values.
Results may differ from the reference program's by a relative error of at most 0.0003.
The reference program's roundings to bfloat16 on the way (of `unit_low` and `weight`) count: a program that leaves them out, or rounds other values in their place, can miss the bound.
Values may be sent and summed in bfloat16 or wider, within the bound.
A program may use at most 128 MiB of HBM per device.

```python
import jax
import jax.numpy as jnp
from jax import lax

D = 128
V_DEV = 192
VIEWS = 6144
N_SUB = 2


def draw_partner(key, part):
    order = jax.random.permutation(key, VIEWS).astype(jnp.int32)
    pairs = order.reshape(VIEWS // 2, 2)
    result = jnp.zeros((VIEWS,), jnp.int32)
    result = result.at[pairs[:, 0]].set(pairs[:, 1])
    result = result.at[pairs[:, 1]].set(pairs[:, 0])
    return result


def steps_of(own_key, dims, split, low, largest):
    factor_of = 1.0
    for axis_at, blocks in split:
        steps = jax.random.uniform(jax.random.fold_in(jax.random.fold_in(own_key, 6), axis_at), (blocks,), jnp.float32, low / len(split), largest / len(split))
        factor_of = factor_of * jnp.repeat(jnp.exp(steps), dims[axis_at] // blocks).reshape((-1,) + (1,) * (len(dims) - 1 - axis_at))
    return factor_of


def scatter_about(rng, extent, scale, limit, pieces=(), kind=jnp.bfloat16):
    entries = scale * jax.random.normal(rng, extent, jnp.float32)
    if pieces:
        entries = entries * steps_of(rng, extent, pieces, -0.22, 0.18)
    return jnp.clip(entries, -limit, limit).astype(kind)


def setup_inputs(seed: int = 0) -> dict:
    streams_of = jax.random.split(jax.random.key(seed), 3)
    projections = scatter_about(streams_of[0], (VIEWS, D), 1.0, 6.0, ((0, 32),), jnp.float32)
    partner = draw_partner(jax.random.fold_in(streams_of[2], 71), 0)
    return {"projections": projections, "partner": partner}


TAU = 0.1
SHIFT = 10.0

def reference(projections, partner):
    inverse = lax.rsqrt(lax.optimization_barrier(jnp.sum(projections * projections, axis=1)) + 1e-06)
    unit = projections * inverse[:, None]
    unit_low = unit.astype(jnp.bfloat16)
    block = V_DEV * N_SUB
    count = VIEWS // block
    columns = jnp.arange(VIEWS, dtype=jnp.int32)

    def scores_of(index):
        start = (index * block).astype(jnp.int32)
        rows_low = lax.dynamic_slice_in_dim(unit_low, start, block, 0)
        score = jnp.dot(rows_low, unit_low.T, preferred_element_type=jnp.float32) / TAU
        rows = start + jnp.arange(block, dtype=jnp.int32)
        diag = columns[None, :] == rows[:, None]
        mates = lax.dynamic_slice_in_dim(partner, start, block, 0)
        hit = columns[None, :] == mates[:, None]
        return (score, diag, hit)

    def forward(index):
        score, diag, hit = scores_of(index)
        total = lax.optimization_barrier(jnp.sum(jnp.where(diag, 0.0, jnp.exp(score - SHIFT)), axis=1))
        lse = jnp.log(total) + SHIFT
        pos = lax.optimization_barrier(jnp.sum(jnp.where(hit, score, 0.0), axis=1))
        return (lse, lse - pos)
    lse, row_loss = lax.map(forward, jnp.arange(count, dtype=jnp.int32))
    lse = lse.reshape(VIEWS)
    row_loss = row_loss.reshape(VIEWS)
    loss = jnp.sum(row_loss) / VIEWS

    def backward(index):
        score, diag, hit = scores_of(index)
        start = (index * block).astype(jnp.int32)
        lse_rows = lax.dynamic_slice_in_dim(lse, start, block, 0)
        weight = jnp.exp(score - lse_rows[:, None]) + jnp.exp(score - lse[None, :])
        weight = weight - 2.0 * hit.astype(jnp.float32)
        weight = jnp.where(diag, 0.0, weight / TAU).astype(jnp.bfloat16)
        return jnp.dot(weight, unit_low, preferred_element_type=jnp.float32)
    grad_unit = lax.map(backward, jnp.arange(count, dtype=jnp.int32)).reshape(VIEWS, D)
    inner = lax.optimization_barrier(jnp.sum(unit * grad_unit, axis=1))
    grad = inverse[:, None] * (grad_unit - unit * inner[:, None])
    return (loss, grad)
```

```python
import functools
import math

import jax
import jax.numpy as jnp
from jax import lax
from jax.experimental import pallas as pl
from jax.experimental.pallas import tpu as pltpu
from jax.sharding import PartitionSpec as P

TAU = 0.1
SHIFT = 10.0
EPS = 1e-06
LANES = 128
MESH = pl.DeviceIdType.MESH
LINE = 4

ORDER = (
    (0, 0, 0), (0, 1, 0), (0, 0, 1), (1, 0, 0), (2, 0, 0), (0, 1, 1), (1, 1, 0), (1, 0, 1),
    (2, 1, 0), (2, 0, 1), (3, 0, 0), (1, 1, 1), (2, 1, 1), (3, 1, 0), (3, 0, 1), (3, 1, 1),
)


def kernel(
    groups, p_hbm, partner_hbm, loss_ref, grad_ref, p_ref, partners,
    blocks, scores, totals, frame, gsum, unit_s, mates, mates_t,
    fetched, send, recv, tsend, trecv, psend, precv, near_in, two_in, three_in,
):
    rows = p_hbm.shape[0]
    pair = 2 * rows
    tiles = pair // LANES
    spare = 2 * LANES - rows
    chips = groups // 2
    d = lax.axis_index("dp")
    c = lax.axis_index("sub")
    z = d // 4
    y = (d // 2) % 2
    x = d % 2
    me = d * 2 + c
    flip = lambda v, n: v + n * (1 - 2 * v)
    inner = ((z + 1) // 2) % 2
    across = 3 - z
    skip = (z + 2) % 4
    places = (
        z,
        z + 1 - 2 * (z % 2),
        inner * across + (1 - inner) * skip,
        inner * skip + (1 - inner) * across,
    )

    def chip_at(chip):
        k, dx, dy = chip
        return places[k] * 4 + flip(y, dy) * 2 + flip(x, dx)

    near_x = (chip_at((0, 1, 0)), c)
    near_y = (chip_at((0, 0, 1)), c)
    diagonal = (chip_at((0, 1, 1)), c)
    mate = (chip_at((1, 0, 0)), c)
    at_across = (across * 4 + y * 2 + x, c)
    at_skip = (skip * 4 + y * 2 + x, c)
    sibling = (d, 1 - c)

    fetch = pltpu.make_async_copy(p_hbm, p_ref, fetched.at[0])
    fetch.start()
    fetch_mates = pltpu.make_async_copy(partner_hbm, partners.at[c], fetched.at[1])
    fetch_mates.start()
    barrier = pltpu.get_barrier_semaphore()
    signal = lambda sem, dev: pl.semaphore_signal(sem, inc=1, device_id=dev, device_id_type=MESH)
    for dev in (near_x, near_y, mate, sibling):
        signal(barrier, dev)

    @pl.when(inner == 1)
    def _():
        signal(barrier, at_across)

    gsum[...] = jnp.zeros_like(gsum)
    fetch.wait()
    p = p_ref[...]
    inverse = lax.rsqrt(jnp.sum(p * p, axis=1, keepdims=True) + EPS)
    unit = p * inverse
    blocks[me] = unit.astype(jnp.bfloat16)
    unit_s[...] = unit
    fetch_mates.wait()
    spread = jnp.broadcast_to(partners[c].astype(jnp.float32), (LANES, rows)).T
    mates[...] = spread.astype(jnp.int32) - lax.broadcasted_iota(jnp.int32, (rows, LANES), 1)

    def copy(b, dev):
        return pltpu.make_async_remote_copy(
            src_ref=blocks.at[b],
            dst_ref=blocks.at[b],
            send_sem=send,
            recv_sem=recv.at[b],
            device_id=dev,
            device_id_type=MESH,
        )

    pl.semaphore_wait(barrier, 4 + inner)
    copy(me, near_x).start()
    copy(me, near_y).start()
    copy(me, mate).start()

    @pl.when(inner == 1)
    def _():
        copy(me, at_across).start()
        signal(two_in, mate)
        signal(two_in, at_across)

    signal(near_in, near_x)
    copy(me, sibling).start()
    swap = pltpu.make_async_remote_copy(
        src_ref=partners.at[c],
        dst_ref=partners.at[c],
        send_sem=psend,
        recv_sem=precv,
        device_id=sibling,
        device_id_type=MESH,
    )
    swap.start()
    pl.semaphore_wait(two_in, 1)

    @pl.when(inner == 1)
    def _():
        signal(three_in, mate)

    copy(me, at_skip).start()
    pl.semaphore_wait(near_in, 1)
    copy(me, diagonal).start()

    @pl.when(inner == 0)
    def _():
        pl.semaphore_wait(three_in, 1)
        copy(me, at_across).start()

    def pair_of(chip):
        return blocks[pl.ds(2 * chip, 2)].reshape(pair, LANES)

    scale = math.log2(math.e) / TAU
    power = lambda dots: jnp.exp2(dots * scale - SHIFT * math.log2(math.e))
    nt = (((1,), (1,)), ((), ()))

    swap.wait_recv()
    copy(d * 2 + 1 - c, sibling).wait_recv()
    both = jnp.concatenate([partners[0], partners[1]], axis=1)
    mates_t[...] = both - lax.broadcasted_iota(jnp.int32, (rows, pair), 0)
    sums = [jnp.zeros((8, pair), jnp.float32), jnp.zeros((8, pair), jnp.float32)]
    fold = lambda v: jnp.sum(v.reshape(rows // 8, 8, pair), axis=0)

    def add(chip):
        b = chip_at(chip) * 2 + c
        dots = lax.dot_general(
            blocks[b], pair_of(d), nt, preferred_element_type=jnp.float32
        )
        powers = power(dots)
        if chip == (0, 0, 0):
            cols = lax.broadcasted_iota(jnp.int32, (rows, pair), 1)
            at = lax.broadcasted_iota(jnp.int32, (rows, pair), 0) + c * rows
            powers = jnp.where(cols == at, 0.0, powers)
        sums[0] = sums[0] + fold(powers)
        sums[1] = sums[1] + fold(jnp.where(mates_t[...] == b * rows, dots, 0.0))

    def keep(chip):
        at_chip = chip_at(chip)
        if chip != (0, 0, 0):
            copy(at_chip * 2 + 1 - c, sibling).wait_recv()
        dots = lax.dot_general(
            blocks[me], pair_of(at_chip), nt, preferred_element_type=jnp.float32
        )
        powers = power(dots)
        if chip == (0, 0, 0):
            cols = lax.broadcasted_iota(jnp.int32, (rows, pair), 1)
            at = lax.broadcasted_iota(jnp.int32, (rows, pair), 0) + c * rows
            powers = jnp.where(cols == at, 0.0, powers)
        scores[ORDER.index(chip)] = powers

    def arrive(chip, *devs):
        b = chip_at(chip) * 2 + c
        copy(b, sibling).wait_recv()
        for dev in devs:
            copy(b, dev).start()
        copy(b, sibling).start()

    add((0, 0, 0))
    arrive((0, 1, 0), mate)
    arrive((0, 0, 1), mate)
    arrive((1, 0, 0))
    keep((0, 0, 0))
    arrive((2, 0, 0), diagonal, near_x, near_y)
    add((0, 1, 0))
    arrive((0, 1, 1), mate)
    add((0, 0, 1))
    add((1, 0, 0))
    add((2, 0, 0))
    arrive((3, 0, 0), diagonal, near_x, near_y)
    add((0, 1, 1))
    add((3, 0, 0))
    keep((0, 1, 0))
    keep((0, 0, 1))
    late = [(1, 1, 0), (1, 0, 1), (2, 1, 0), (2, 0, 1), (1, 1, 1), (2, 1, 1), (3, 1, 0), (3, 0, 1), (3, 1, 1)]
    fill = [(1, 0, 0), (2, 0, 0), (0, 1, 1), (3, 0, 0)]
    for n, chip in enumerate(late):
        arrive(chip)
        add(chip)
        if n < len(fill):
            keep(fill[n])

    found = jnp.sum(sums[1], axis=0, keepdims=True)
    totals[me, :, 0:pair] = jnp.sum(sums[0], axis=0, keepdims=True)
    totals[me, :, pair : pair + LANES] = (
        sum(found[:, t * LANES : (t + 1) * LANES] for t in range(tiles)) / TAU
    )

    def share(dev):
        return pltpu.make_async_remote_copy(
            src_ref=totals.at[me],
            dst_ref=totals.at[me],
            send_sem=tsend,
            recv_sem=trecv.at[d],
            device_id=dev,
            device_id_type=MESH,
        )

    for chip in ORDER[::-1]:
        if chip != (0, 0, 0):
            share((chip_at(chip), c)).start()
        share((chip_at(chip), 1 - c)).start()

    def shared(chip):
        at = totals.at[d * 2 + 1 - c] if chip == (0, 0, 0) else totals.at[pl.ds(2 * chip_at(chip), 2)]
        return pltpu.make_async_remote_copy(
            src_ref=at,
            dst_ref=at,
            send_sem=tsend,
            recv_sem=trecv.at[chip_at(chip)],
            device_id=sibling,
            device_id_type=MESH,
        )

    for chip in late:
        keep(chip)

    logs = jnp.zeros((1, pair), jnp.float32)
    matched = jnp.zeros((1, LANES), jnp.float32)
    for chip in ORDER:
        at_chip = chip_at(chip)
        shared(chip).wait_recv()
        a, b = totals[2 * at_chip], totals[2 * at_chip + 1]
        column = a[:, :pair] + b[:, :pair]
        logs = logs + jnp.log(column)
        matched = matched + a[:, pair:] + b[:, pair:]
        if chip == (0, 0, 0):
            own = jnp.where(c == 0, column[:, : 2 * LANES], column[:, pair - 2 * LANES :])
            frame[...] = jnp.broadcast_to((1.0 / TAU) / own, (LANES, 2 * LANES)).T
            row_scale = frame[pl.ds(pl.multiple_of(c * spare, 8), rows), :]
        powers = scores[ORDER.index(chip)]
        col_scale = (1.0 / TAU) / column
        parts = []
        for t in range(tiles):
            part = slice(t * LANES, (t + 1) * LANES)
            weight = powers[:, part] * (row_scale + col_scale[:, part])
            hit = mates[...] == at_chip * pair + t * LANES
            parts.append(jnp.where(hit, weight - 2.0 / TAU, weight).astype(jnp.bfloat16))
        gsum[...] += jnp.dot(
            jnp.concatenate(parts, axis=1), pair_of(at_chip), preferred_element_type=jnp.float32
        )

    grown = gsum[...]
    unit = unit_s[...]
    p = p_ref[...]
    inverse = lax.rsqrt(jnp.sum(p * p, axis=1, keepdims=True) + EPS)
    inner_product = jnp.sum(unit * grown, axis=1, keepdims=True)
    grad_ref[...] = inverse * (grown - unit * inner_product)
    loss_ref[0, 0] = (jnp.sum(logs) - jnp.sum(matched)) / (rows * groups) + SHIFT

    swap.wait_send()
    sent = blocks.at[pl.ds(0, groups - 1)]
    pltpu.make_async_remote_copy(
        src_ref=sent, dst_ref=sent, send_sem=send, recv_sem=recv.at[0], device_id=sibling,
        device_id_type=MESH,
    ).wait_send()
    told = totals.at[pl.ds(0, groups - 1)]
    pltpu.make_async_remote_copy(
        src_ref=told, dst_ref=told, send_sem=tsend, recv_sem=trecv.at[0], device_id=sibling,
        device_id_type=MESH,
    ).wait_send()


def fused(projections, partner):
    rows, width = projections.shape
    groups = lax.axis_size(("dp", "sub"))
    chips = groups // 2
    pair = 2 * rows
    loss, grad = pl.pallas_call(
        functools.partial(kernel, groups),
        out_shape=(
            jax.ShapeDtypeStruct((1, 1), jnp.float32),
            jax.ShapeDtypeStruct((rows, width), jnp.float32),
        ),
        in_specs=[pl.BlockSpec(memory_space=pl.ANY)] * 2,
        out_specs=(
            pl.BlockSpec(memory_space=pltpu.SMEM),
            pl.BlockSpec(memory_space=pltpu.VMEM),
        ),
        scratch_shapes=[
            pltpu.VMEM((rows, width), jnp.float32),
            pltpu.VMEM((2, 1, rows), jnp.int32),
            pltpu.VMEM((groups, rows, width), jnp.bfloat16),
            pltpu.VMEM((chips, rows, pair), jnp.float32),
            pltpu.VMEM((groups, 1, pair + LANES), jnp.float32),
            pltpu.VMEM((2 * LANES, LANES), jnp.float32),
            pltpu.VMEM((rows, width), jnp.float32),
            pltpu.VMEM((rows, width), jnp.float32),
            pltpu.VMEM((rows, LANES), jnp.int32),
            pltpu.VMEM((rows, pair), jnp.int32),
            pltpu.SemaphoreType.DMA((2,)),
            pltpu.SemaphoreType.DMA,
            pltpu.SemaphoreType.DMA((groups,)),
            pltpu.SemaphoreType.DMA,
            pltpu.SemaphoreType.DMA((chips,)),
            pltpu.SemaphoreType.DMA,
            pltpu.SemaphoreType.DMA,
            pltpu.SemaphoreType.REGULAR,
            pltpu.SemaphoreType.REGULAR,
            pltpu.SemaphoreType.REGULAR,
        ],
        compiler_params=pltpu.CompilerParams(collective_id=0, has_side_effects=True),
    )(projections, partner.reshape(1, rows))
    return loss.reshape(()), grad


def general(projections, partner):
    rows = projections.shape[0]
    axes = ("dp", "sub")
    inverse = lax.rsqrt(jnp.sum(projections * projections, axis=1) + EPS)
    unit = projections * inverse[:, None]
    low = unit.astype(jnp.bfloat16)
    everyone = lax.all_gather(low, axes, axis=0, tiled=True)
    columns = jnp.arange(everyone.shape[0], dtype=jnp.int32)
    ids = lax.axis_index(axes) * rows + jnp.arange(rows, dtype=jnp.int32)
    score = (
        lax.dot_general(
            low, everyone, (((1,), (1,)), ((), ())), preferred_element_type=jnp.float32
        )
        / TAU
    )
    diag = columns[None, :] == ids[:, None]
    hit = columns[None, :] == partner[:, None]
    total = jnp.sum(jnp.where(diag, 0.0, jnp.exp(score - SHIFT)), axis=1)
    found = jnp.sum(jnp.where(hit, score, 0.0), axis=1)
    lse = jnp.log(total) + SHIFT
    lse_all = lax.all_gather(lse, axes, axis=0, tiled=True)
    loss = lax.psum(jnp.sum(lse - found), axes) / everyone.shape[0]
    weight = jnp.exp(score - lse[:, None]) + jnp.exp(score - lse_all[None, :])
    weight = weight - 2.0 * hit.astype(jnp.float32)
    weight = jnp.where(diag, 0.0, weight / TAU).astype(jnp.bfloat16)
    grown = jnp.dot(weight, everyone, preferred_element_type=jnp.float32)
    inner = jnp.sum(unit * grown, axis=1)
    return loss, inverse[:, None] * (grown - unit * inner[:, None])


def solution(mesh):
    small = mesh.shape["dp"] == 4 * LINE and mesh.shape["sub"] == 2

    def body(projections, partner):
        rows, width = projections.shape
        fits = width == LANES and LANES < rows < 2 * LANES and (2 * rows) % LANES == 0
        return (fused if small and fits else general)(projections, partner)

    return jax.shard_map(
        body,
        mesh=mesh,
        in_specs=(P(("dp", "sub"), None), P(("dp", "sub"))),
        out_specs=(P(), P(("dp", "sub"), None)),
        check_vma=False,
    )
```
